32 devices in a mesh: grp: 4 (over z), blk: 4 (over x, core), tp: 2 (over y).
Axes of the slice: x: 2, y: 2, z: 4, core: 2. Of those that a mesh axis runs over, the one named last changes fastest.
Arguments:
- queries: bfloat16 [512, 4096], P('grp', ('blk', 'tp')), may hold values from -110 to 110
- keys: bfloat16 [512, 4096], P('grp', ('blk', 'tp')), may hold values from -5 to 5
- values: bfloat16 [512, 4096], P('grp', ('blk', 'tp')), may hold values from -6 to 6
- cross_queries: bfloat16 [512, 4096], P('grp', ('blk', 'tp')), may hold values from -110 to 110
- history_keys: bfloat16 [768, 4096], P('grp', ('blk', 'tp')), may hold values from -5 to 5
- history_values: bfloat16 [768, 4096], P('grp', ('blk', 'tp')), may hold values from -6 to 6
- frame_ids: int32 [512], replicated, may hold values from 0 to 7, never falling along the last dimension, each value on 1 to 128 neighbouring positions
- masked: int32 [512], replicated, may hold values 0 or 1
- out_weight: bfloat16 [4096, 5120], P(('blk', 'tp')), may hold values from -0.09375 to 0.09375
- cotangent: bfloat16 [512, 5120], P('grp', ('blk', 'tp')), may hold values from -6 to 6
Outputs:
- layer_out: bfloat16 [512, 5120], P('grp', ('blk', 'tp'))
- query_grad: bfloat16 [512, 4096], P('grp', ('blk', 'tp'))
- key_grad: bfloat16 [512, 4096], P('grp', ('blk', 'tp'))
- value_grad: bfloat16 [512, 4096], P('grp', ('blk', 'tp'))
- cross_query_grad: bfloat16 [512, 4096], P('grp', ('blk', 'tp'))
- history_key_grad: bfloat16 [768, 4096], P('grp', ('blk', 'tp'))
- history_value_grad: bfloat16 [768, 4096], P('grp', ('blk', 'tp'))
- weight_grad: float32 [4096, 5120], P(('blk', 'tp'), 'grp')
The draws below stay inside these ranges and needn't reach their ends.
Inputs may be any that keep to these rules, and one draw needn't show every extreme that they name: `frame_ids`: frame numbers never fall along the tokens; a frame holds 1 to 128 tokens.
All inputs are finite; a program needn't handle non-finite values.
Results may differ from the reference program's by a relative error of at most 0.017.
Values may be sent and summed in bfloat16 or wider, within the bound.
No kernel may reach another device: no remote copies, remote signals or barrier semaphores. Data moves between devices by JAX's collectives and lax.ppermute only.
A program may use at most 128 MiB of HBM per device.

```python
import math
import jax
import jax.numpy as jnp
import numpy as np
from jax import lax

D = 5120
HEADS = 32
HD = 128
TOKENS = 512
HISTORY = 768
FRAMES = 8
FRAME_MOST = 128


def self_pair(key):
    base = jax.random.fold_in(key, 101)
    key_query, key_key = jax.random.split(base, 2)
    width = HEADS * HD
    keys_all = jnp.clip(jax.random.normal(key_key, (TOKENS, width), jnp.float32), -4.5, 4.5)
    queries_all = jnp.clip(jax.random.normal(key_query, (TOKENS, width), jnp.float32), -4.5, 4.5)
    return (queries_all, keys_all)


def cross_pair(key):
    base = jax.random.fold_in(key, 202)
    key_query, key_key = jax.random.split(base, 2)
    width = HEADS * HD
    memory = jnp.clip(jax.random.normal(key_key, (HISTORY, width), jnp.float32), -4.5, 4.5)
    asking = jnp.clip(jax.random.normal(key_query, (TOKENS, width), jnp.float32), -4.5, 4.5)
    return (asking, memory)


def draw_queries(key, part):
    return self_pair(key)[0].astype(jnp.bfloat16)


def draw_keys(key, part):
    return self_pair(key)[1].astype(jnp.bfloat16)


def draw_cross_queries(key, part):
    return cross_pair(key)[0].astype(jnp.bfloat16)


def draw_history_keys(key, part):
    return cross_pair(key)[1].astype(jnp.bfloat16)


def place_ends(drawn, rng, smallest, high):
    index_at = [jax.random.randint(jax.random.fold_in(rng, axis), (), 0, length) for axis, length in enumerate(drawn.shape)]
    longest = drawn.shape.index(max(drawn.shape))
    neighbour = index_at[:longest] + [(index_at[longest] + 1) % drawn.shape[longest]] + index_at[longest + 1:]
    return drawn.at[tuple(index_at)].set(smallest).at[tuple(neighbour)].set(high)


def strengthened(array, rng, source, target, blocks, factor):
    def block_of(axis_at):
        return (jnp.arange(array.shape[axis_at]) // (array.shape[axis_at] // blocks)).reshape((-1,) + (1,) * (array.ndim - 1 - axis_at))

    first = jax.random.permutation(rng, blocks)[block_of(target)]
    other_side = (block_of(target) + blocks // 2) % blocks
    return jnp.where((block_of(source) == first) | (block_of(source) == other_side), factor * array, array)


def level_of(key, shape, cuts, smallest, high):
    level, own = 1.0, jax.random.fold_in(key, 6)
    for dim, parts in cuts:
        heights = jnp.exp(jax.random.uniform(jax.random.fold_in(own, dim), (parts,), jnp.float32, smallest / len(cuts), high / len(cuts)))
        level = level * jnp.repeat(heights, shape[dim] // parts).reshape([-1 if axis == dim else 1 for axis in range(len(shape))])
    return level


def split_up(number_of, total, limit, lean):
    weights = [(1 << 20) // math.isqrt(grade ** lean) + 1 for grade in range(2, number_of + 1)]
    rest, counts = total - limit - (number_of - 1), [1] * (number_of - 1)
    while rest > 0:
        candidates = [i for i in range(number_of - 1) if counts[i] < limit]
        mass, remaining = sum([weights[i] for i in candidates]), rest
        for i in candidates:
            more = min(limit - counts[i], max(1, remaining * weights[i] // mass), rest)
            counts[i] = counts[i] + more
            rest = rest - more
    return np.array([limit] + counts)


def uneven_parts(rng, number_of, total, most, skew):
    if number_of == 2:
        one = jax.random.randint(rng, (), max(1, total - most), min(most, total - 1) + 1)
        return jnp.stack([one, total - one])
    sizes = jnp.asarray(split_up(number_of, total, most, skew), jnp.int32)
    couples = (number_of - 1) // 2
    donor, taker = sizes[1:1 + 2 * couples:2], sizes[2:2 + 2 * couples:2]
    room = jnp.minimum(donor - 1, most - taker)
    passed = jax.random.randint(jax.random.fold_in(rng, 1), (couples,), 0, 1 << 20) % (room + 1)
    sizes = sizes.at[1:1 + 2 * couples:2].set(donor - passed).at[2:2 + 2 * couples:2].set(taker + passed)
    return sizes[jax.random.permutation(jax.random.fold_in(rng, 2), number_of)]


def normal_values(rng, shape, deviation, most, pieces=(), kind=jnp.bfloat16):
    array = deviation * jax.random.normal(rng, shape, jnp.float32)
    if pieces:
        array = array * level_of(rng, shape, pieces, -0.22, 0.18)
    return jnp.clip(array, -most, most).astype(kind)


def noise_with(key, shape, scale, most, pieces, heavy, kind=jnp.bfloat16):
    drawn = scale * jax.random.normal(key, shape, jnp.float32)
    if pieces:
        drawn = drawn * level_of(key, shape, pieces, -0.22, 0.18)
    return jnp.clip(strengthened(drawn, jax.random.fold_in(key, 3), *heavy), -most, most).astype(kind)


def setup_inputs(seed: int = 0) -> dict:
    splits = jax.random.split(jax.random.key(seed), 11)
    return {
        "queries": draw_queries(jax.random.fold_in(splits[10], 71), 0),
        "keys": draw_keys(jax.random.fold_in(splits[10], 71), 0),
        "values": normal_values(splits[2], (TOKENS, HEADS * HD), 1.0, 6.0, ((0, 4), (1, 8))),
        "cross_queries": draw_cross_queries(jax.random.fold_in(splits[10], 71), 0),
        "history_keys": draw_history_keys(jax.random.fold_in(splits[10], 71), 0),
        "history_values": normal_values(splits[5], (HISTORY, HEADS * HD), 1.0, 6.0, ((0, 4), (1, 8))),
        "frame_ids": jnp.searchsorted(jnp.cumsum(uneven_parts(splits[6], FRAMES, TOKENS, FRAME_MOST, 1)), jnp.arange(TOKENS), side="right").astype(jnp.int32),
        "masked": place_ends((jax.random.randint(splits[7], (TOKENS,), 0, 2) < 1).astype(jnp.int32), jax.random.fold_in(splits[7], 1), 0, 1),
        "out_weight": normal_values(splits[8], (HEADS * HD, D), (HEADS * HD) ** -0.5, 0.09375, ((0, 8),)),
        "cotangent": noise_with(splits[9], (TOKENS, D), 1.0, 6.0, ((0, 4), (1, 8)), (0, 1, 8, 2.0)),
    }


def normalize(score):
    highest = jnp.max(score, axis=-1, keepdims=True)
    weights = jnp.exp(score - highest)
    return weights / jnp.sum(weights, axis=-1, keepdims=True)


def head_slice(matrix, head):
    return lax.dynamic_slice_in_dim(matrix, head * HD, HD, 1)


def head_probs(queries, keys, cross_queries, history_keys, allowed, head):
    factor = HD ** -0.5
    self_score = jnp.dot(head_slice(queries, head), head_slice(keys, head).T, preferred_element_type=jnp.float32) * factor
    self_prob = normalize(jnp.where(allowed, self_score, -jnp.inf))
    cross_score = jnp.dot(head_slice(cross_queries, head), head_slice(history_keys, head).T, preferred_element_type=jnp.float32) * factor
    return self_prob, normalize(cross_score)


def flatten(stacked):
    return jnp.transpose(stacked, (1, 0, 2)).reshape(stacked.shape[1], HEADS * HD)


def reference(queries, keys, values, cross_queries, history_keys, history_values, frame_ids, masked, out_weight, cotangent):
    factor = HD ** -0.5
    positions = jnp.arange(TOKENS, dtype=jnp.int32)
    causal = frame_ids[None, :] <= frame_ids[:, None]
    allowed = causal & ((masked[None, :] == 0) | (positions[None, :] == positions[:, None]))
    head_ids = jnp.arange(HEADS, dtype=jnp.int32)

    def forward_head(head):
        self_prob, cross_prob = head_probs(queries, keys, cross_queries, history_keys, allowed, head)
        self_out = jnp.dot(self_prob.astype(jnp.bfloat16), head_slice(values, head), preferred_element_type=jnp.float32)
        cross_out = jnp.dot(cross_prob.astype(jnp.bfloat16), head_slice(history_values, head), preferred_element_type=jnp.float32)
        return self_out + cross_out

    attended = flatten(lax.map(forward_head, head_ids)).astype(jnp.bfloat16)
    layer_out = jnp.dot(attended, out_weight, preferred_element_type=jnp.float32).astype(jnp.bfloat16)
    grad_attended = jnp.dot(cotangent, out_weight.T, preferred_element_type=jnp.float32).astype(jnp.bfloat16)
    weight_grad = jnp.dot(attended.T, cotangent, preferred_element_type=jnp.float32)

    def backward_head(head):
        self_prob, cross_prob = head_probs(queries, keys, cross_queries, history_keys, allowed, head)
        grad_head = head_slice(grad_attended, head)
        self_dprob = jnp.dot(grad_head, head_slice(values, head).T, preferred_element_type=jnp.float32)
        self_dot = jnp.sum(self_prob * self_dprob, axis=-1, keepdims=True)
        self_dscore = (self_prob * (self_dprob - self_dot)).astype(jnp.bfloat16)
        cross_dprob = jnp.dot(grad_head, head_slice(history_values, head).T, preferred_element_type=jnp.float32)
        cross_dot = jnp.sum(cross_prob * cross_dprob, axis=-1, keepdims=True)
        cross_dscore = (cross_prob * (cross_dprob - cross_dot)).astype(jnp.bfloat16)
        query_part = jnp.dot(self_dscore, head_slice(keys, head), preferred_element_type=jnp.float32) * factor
        key_part = jnp.dot(self_dscore.T, head_slice(queries, head), preferred_element_type=jnp.float32) * factor
        value_part = jnp.dot(self_prob.astype(jnp.bfloat16).T, grad_head, preferred_element_type=jnp.float32)
        cross_part = jnp.dot(cross_dscore, head_slice(history_keys, head), preferred_element_type=jnp.float32) * factor
        memory_part = jnp.dot(cross_dscore.T, head_slice(cross_queries, head), preferred_element_type=jnp.float32) * factor
        recall_part = jnp.dot(cross_prob.astype(jnp.bfloat16).T, grad_head, preferred_element_type=jnp.float32)
        return query_part, key_part, value_part, cross_part, memory_part, recall_part

    gradients = lax.map(backward_head, head_ids)
    query_grad, key_grad, value_grad, cross_query_grad, history_key_grad, history_value_grad = [flatten(member).astype(jnp.bfloat16) for member in gradients]
    return (layer_out, query_grad, key_grad, value_grad, cross_query_grad, history_key_grad, history_value_grad, weight_grad)
```

```python
import jax
import jax.numpy as jnp
from jax import lax
from jax.sharding import PartitionSpec as P

HD = 128


def split_heads(matrix):
    return matrix.reshape(matrix.shape[0], matrix.shape[1] // HD, HD)


def merge_heads(tensor):
    return tensor.reshape(tensor.shape[0], tensor.shape[1] * tensor.shape[2])


def visible(query_frames, key_frames, key_masked, query_index, key_index):
    causal = key_frames[None, :] <= query_frames[:, None]
    open_key = (key_masked[None, :] == 0) | (key_index[None, :] == query_index[:, None])
    return causal & open_key


def scores_of(query_split, key_split, factor):
    return (
        jnp.einsum("qhd,khd->hqk", query_split, key_split, preferred_element_type=jnp.float32)
        * factor
    )


def softmax_parts(score):
    highest = jnp.max(score, axis=-1, keepdims=True)
    weights = jnp.exp(score - highest)
    summed = jnp.sum(weights, axis=-1, keepdims=True)
    return (weights / summed, highest[..., 0] + jnp.log(summed[..., 0]))


def key_side(dscore, prob_low, query_split, grad_split, factor):
    key_part = merge_heads(
        jnp.einsum("hqk,qhd->khd", dscore, query_split, preferred_element_type=jnp.float32) * factor
    )
    value_part = merge_heads(
        jnp.einsum("hqk,qhd->khd", prob_low, grad_split, preferred_element_type=jnp.float32)
    )
    return (key_part, value_part)


def on_device_tokens(
    queries,
    keys,
    values,
    cross_queries,
    history_keys,
    history_values,
    frame_ids,
    masked,
    out_weight,
    cotangent,
):
    row_count = queries.shape[0]
    factor = HD ** (-0.5)
    row_start = lax.axis_index("grp") * row_count
    query_index = row_start + jnp.arange(row_count, dtype=jnp.int32)
    every_key, every_value, past_keys, past_values = (
        lax.all_gather(keys, "grp", axis=0, tiled=True),
        lax.all_gather(values, "grp", axis=0, tiled=True),
        lax.all_gather(history_keys, "grp", axis=0, tiled=True),
        lax.all_gather(history_values, "grp", axis=0, tiled=True),
    )
    key_index = jnp.arange(every_key.shape[0], dtype=jnp.int32)
    query_frames = lax.dynamic_slice_in_dim(frame_ids, row_start, row_count)
    allowed = visible(query_frames, frame_ids, masked, query_index, key_index)
    query_split = split_heads(queries)
    cross_split = split_heads(cross_queries)
    key_split = split_heads(every_key)
    value_split = split_heads(every_value)
    memory_split = split_heads(past_keys)
    recall_split = split_heads(past_values)
    self_score = jnp.where(allowed[None], scores_of(query_split, key_split, factor), -jnp.inf)
    self_prob, self_log = softmax_parts(self_score)
    cross_prob, cross_log = softmax_parts(scores_of(cross_split, memory_split, factor))
    self_low = self_prob.astype(jnp.bfloat16)
    cross_low = cross_prob.astype(jnp.bfloat16)
    combined = jnp.einsum("hqk,khd->qhd", self_low, value_split, preferred_element_type=jnp.float32)
    combined = combined + jnp.einsum(
        "hqk,khd->qhd", cross_low, recall_split, preferred_element_type=jnp.float32
    )
    attended = merge_heads(combined).astype(jnp.bfloat16)
    head_terms = jnp.dot(attended, out_weight, preferred_element_type=jnp.float32)
    layer_out = lax.psum_scatter(head_terms, ("blk", "tp"), scatter_dimension=1, tiled=True).astype(
        jnp.bfloat16
    )
    arrived = lax.all_gather(cotangent, ("blk", "tp"), axis=1, tiled=True)
    grad_rows = lax.dot_general(
        arrived, out_weight, (((1,), (1,)), ((), ())), preferred_element_type=jnp.float32
    )
    product = lax.dot_general(
        attended, arrived, (((0,), (0,)), ((), ())), preferred_element_type=jnp.float32
    )
    grad_cols = product
    grad_rows, grad_cols = (grad_rows, grad_cols)
    weight_grad = lax.psum_scatter(
        grad_cols.astype(jnp.bfloat16), "grp", scatter_dimension=1, tiled=True
    ).astype(jnp.float32)
    grad_low = grad_rows.astype(jnp.bfloat16)
    grad_split = split_heads(grad_low)
    self_dprob = jnp.einsum(
        "qhd,khd->hqk", grad_split, value_split, preferred_element_type=jnp.float32
    )
    self_dot = jnp.sum(self_prob * self_dprob, axis=-1)
    self_dscore = (self_prob * (self_dprob - self_dot[..., None])).astype(jnp.bfloat16)
    cross_dprob = jnp.einsum(
        "qhd,khd->hqk", grad_split, recall_split, preferred_element_type=jnp.float32
    )
    cross_dot = jnp.sum(cross_prob * cross_dprob, axis=-1)
    cross_dscore = (cross_prob * (cross_dprob - cross_dot[..., None])).astype(jnp.bfloat16)
    query_grad = merge_heads(
        jnp.einsum("hqk,khd->qhd", self_dscore, key_split, preferred_element_type=jnp.float32)
        * factor
    ).astype(jnp.bfloat16)
    cross_grad = merge_heads(
        jnp.einsum("hqk,khd->qhd", cross_dscore, memory_split, preferred_element_type=jnp.float32)
        * factor
    ).astype(jnp.bfloat16)
    asked, asked_cross, asked_grad = (
        lax.all_gather(queries, "grp", axis=0, tiled=True),
        lax.all_gather(cross_queries, "grp", axis=0, tiled=True),
        lax.all_gather(grad_low, "grp", axis=0, tiled=True),
    )
    self_dots, cross_dots, self_logs, cross_logs = (
        lax.all_gather(self_dot, "grp", axis=1, tiled=True),
        lax.all_gather(cross_dot, "grp", axis=1, tiled=True),
        lax.all_gather(self_log, "grp", axis=1, tiled=True),
        lax.all_gather(cross_log, "grp", axis=1, tiled=True),
    )
    own_masked = lax.dynamic_slice_in_dim(masked, row_start, row_count)
    allowed_own = visible(frame_ids, query_frames, own_masked, key_index, query_index)
    asked_split = split_heads(asked)
    cross_every = split_heads(asked_cross)
    grad_every = split_heads(asked_grad)
    score_own = jnp.where(
        allowed_own[None], scores_of(asked_split, split_heads(keys), factor), -jnp.inf
    )
    prob_own = jnp.exp(score_own - self_logs[..., None])
    dprob_own = jnp.einsum(
        "qhd,khd->hqk", grad_every, split_heads(values), preferred_element_type=jnp.float32
    )
    dscore_own = (prob_own * (dprob_own - self_dots[..., None])).astype(jnp.bfloat16)
    key_part, value_part = key_side(
        dscore_own, prob_own.astype(jnp.bfloat16), asked_split, grad_every, factor
    )
    prob_past = jnp.exp(
        scores_of(cross_every, split_heads(history_keys), factor) - cross_logs[..., None]
    )
    dprob_past = jnp.einsum(
        "qhd,khd->hqk", grad_every, split_heads(history_values), preferred_element_type=jnp.float32
    )
    dscore_past = (prob_past * (dprob_past - cross_dots[..., None])).astype(jnp.bfloat16)
    memory_part, recall_part = key_side(
        dscore_past, prob_past.astype(jnp.bfloat16), cross_every, grad_every, factor
    )
    key_grad = key_part.astype(jnp.bfloat16)
    value_grad = value_part.astype(jnp.bfloat16)
    history_key_grad = memory_part.astype(jnp.bfloat16)
    history_value_grad = recall_part.astype(jnp.bfloat16)
    return (
        layer_out,
        query_grad,
        key_grad,
        value_grad,
        cross_grad,
        history_key_grad,
        history_value_grad,
        weight_grad,
    )


def rotated(slots, me):
    n = len(slots)
    twice = jnp.stack(slots[::-1] + slots[::-1])
    return lax.dynamic_slice_in_dim(twice, n - 1 - me, n, axis=0)


def shifted(piece, axis, shift, size):
    return lax.ppermute(piece, axis, [(i, (i + shift) % size) for i in range(size)])


def flipped(piece, axis, bit, size):
    return lax.ppermute(piece, axis, [(i, i ^ bit) for i in range(size)])


def ordered(flag, own, other):
    return jnp.where(flag == 0, jnp.concatenate([own, other]), jnp.concatenate([other, own]))


def plane_gather(piece, blk_size, tp_size):
    blk, tp = lax.axis_index("blk"), lax.axis_index("tp")
    steps = [(bit, shift) for bit in range(0, blk_size, 2) for shift in range(tp_size) if bit or shift]
    got = {(0, 0): piece}
    for bit, shift in steps:
        pairs = []
        for b in range(blk_size):
            for t in range(tp_size):
                pairs.append((b * tp_size + t, (b ^ bit) * tp_size + (t + shift) % tp_size))
        got[(bit, shift)] = lax.ppermute(piece, ("blk", "tp"), pairs)
    rows = [
        rotated([got[(bit, shift)] for shift in range(tp_size)], tp) for bit in range(0, blk_size, 2)
    ]
    level = 2
    while level < blk_size:
        flag = (blk // level) % 2
        rows = [
            ordered(flag, rows[2 * i], rows[2 * i + 1]) for i in range(len(rows) // 2)
        ]
        level *= 2
    half = rows[0].reshape((blk_size // 2, tp_size) + piece.shape)
    other = flipped(half, "blk", 1, blk_size)
    flag = blk % 2
    both = jnp.where(
        flag == 0, jnp.stack([half, other], axis=1), jnp.stack([other, half], axis=1)
    )
    return both.reshape((blk_size * tp_size,) + piece.shape)


def on_device_heads(
    grp, blk_size, tp_size, queries, keys, values, cross_queries, history_keys, history_values,
    frame_ids, masked, out_weight, cotangent,
):
    bf16, f32 = jnp.bfloat16, jnp.float32
    factor = HD ** (-0.5)
    me = lax.axis_index("grp")
    plane = lax.axis_index("blk") * tp_size + lax.axis_index("tp")
    plane_size = blk_size * tp_size
    row_count, width = queries.shape
    past_count = history_keys.shape[0]
    own_width = width // grp
    heads = own_width // HD
    sources = [queries, keys, values, cross_queries, history_keys, history_values]

    def columns(array, rank):
        return lax.dynamic_slice_in_dim(array, rank * own_width, own_width, 1)

    def outgoing(shift):
        rank = (me + shift) % grp
        return jnp.concatenate([columns(array, rank) for array in sources])

    came = [outgoing(0)] + [shifted(outgoing(s), "grp", s, grp) for s in range(1, grp)]
    lengths = [row_count] * 4 + [past_count] * 2
    starts = [sum(lengths[:i]) for i in range(6)]

    arrived = plane_gather(cotangent, blk_size, tp_size)
    cot_rows = jnp.moveaxis(arrived, 0, 1).reshape(row_count, -1)
    grad_rows = lax.dot_general(
        cot_rows, out_weight, (((1,), (1,)), ((), ())), preferred_element_type=f32
    ).astype(bf16)
    cot_width = cot_rows.shape[1] // grp
    part_rows = row_count // plane_size
    cot_part = lax.dynamic_slice_in_dim(cot_rows, plane * part_rows, part_rows, 0)

    def grad_out(shift):
        rank = (me + shift) % grp
        piece = lax.dynamic_slice_in_dim(cot_part, rank * cot_width, cot_width, 1)
        piece = piece.reshape(part_rows, cot_width // own_width, own_width).swapaxes(0, 1)
        return jnp.concatenate([columns(grad_rows, rank), piece.reshape(-1, own_width)])

    grads = [grad_out(0)] + [shifted(grad_out(s), "grp", s, grp) for s in range(1, grp)]
    grad_head = jnp.concatenate([piece[:row_count] for piece in grads])
    cot_mine = rotated([piece[row_count:] for piece in grads], me)
    cot_mine = cot_mine.reshape(grp, cot_width // own_width, part_rows, own_width)
    cot_mine = cot_mine.swapaxes(1, 2).reshape(grp, part_rows, cot_width)
    cot_all = plane_gather(cot_mine.reshape(grp * part_rows, cot_width), blk_size, tp_size)
    cot_all = cot_all.reshape(plane_size, grp, part_rows, cot_width).swapaxes(0, 1)
    cot_all = cot_all.reshape(grp * row_count, cot_width)

    def part(index):
        return split_heads(
            jnp.concatenate([piece[starts[index] : starts[index] + lengths[index]] for piece in came])
        )

    q, k, v, cq, hk, hv = [part(index) for index in range(6)]
    slot_rank = (me - jnp.arange(grp, dtype=jnp.int32)) % grp
    token = (slot_rank[:, None] * row_count + jnp.arange(row_count, dtype=jnp.int32)).reshape(-1)

    def by_slot(vector):
        parts = vector.reshape(grp, row_count)
        return jnp.concatenate(
            [lax.dynamic_index_in_dim(parts, (me - s) % grp, 0, keepdims=False) for s in range(grp)]
        )

    frames, hidden = by_slot(frame_ids), by_slot(masked)
    allowed = visible(frames, frames, hidden, token, token)

    def forward(query, key, limit):
        score = scores_of(query, key, factor)
        if limit is not None:
            score = jnp.where(limit[None], score, -jnp.inf)
        highest = jnp.max(score, axis=-1, keepdims=True)
        weights = jnp.exp(score - highest)
        return weights / jnp.sum(weights, axis=-1, keepdims=True)

    self_prob = forward(q, k, allowed)
    cross_prob = forward(cq, hk, None)
    self_low, cross_low = self_prob.astype(bf16), cross_prob.astype(bf16)
    combined = jnp.einsum("hqk,khd->qhd", self_low, v, preferred_element_type=f32)
    combined = combined + jnp.einsum("hqk,khd->qhd", cross_low, hv, preferred_element_type=f32)
    attended = merge_heads(combined).astype(bf16).reshape(grp, row_count, own_width)
    attended = rotated([attended[s] for s in range(grp)], me).reshape(grp * row_count, own_width)

    spread = [attended] + [shifted(attended, "grp", s, grp) for s in range(1, grp)]
    att_heads = rotated(spread, me)
    att_own = lax.dynamic_slice_in_dim(att_heads, me * row_count, row_count, 1)
    att_own = att_own.swapaxes(0, 1).reshape(row_count, width)

    gs = split_heads(grad_head)

    def backward(prob, low, query, key, value):
        dprob = jnp.einsum("qhd,khd->hqk", gs, value, preferred_element_type=f32)
        dot = jnp.sum(prob * dprob, axis=-1, keepdims=True)
        dscore = (prob * (dprob - dot)).astype(bf16)
        dq = jnp.einsum("hqk,khd->qhd", dscore, key, preferred_element_type=f32) * factor
        dk, dv = key_side(dscore, low, query, gs, factor)
        return merge_heads(dq).astype(bf16), dk.astype(bf16), dv.astype(bf16)

    dq, dk, dv = backward(self_prob, self_low, q, k, v)
    dcq, dhk, dhv = backward(cross_prob, cross_low, cq, hk, hv)
    results = [dq, dk, dv, dcq, dhk, dhv]

    def returned(slot):
        return jnp.concatenate(
            [array[slot * size : (slot + 1) * size] for array, size in zip(results, lengths)]
        )

    back = [returned(0)] + [shifted(returned(s), "grp", -s, grp) for s in range(1, grp)]
    twice = jnp.stack(back + back)
    back = lax.dynamic_slice_in_dim(twice, (grp - me) % grp, grp, axis=0)

    def restored(index):
        piece = back[:, starts[index] : starts[index] + lengths[index]]
        return piece.swapaxes(0, 1).reshape(lengths[index], width)

    query_grad, key_grad, value_grad, cross_grad, hk_grad, hv_grad = [
        restored(index) for index in range(6)
    ]

    weight_grad = jnp.einsum("gtf,tc->gfc", att_heads, cot_all, preferred_element_type=f32)
    weight_grad = weight_grad.reshape(width, cot_width)

    terms = jnp.dot(att_own, out_weight, preferred_element_type=f32).astype(bf16)
    blocks = terms.reshape(row_count, blk_size // 2, 2, tp_size, -1).transpose(2, 1, 3, 0, 4)
    low_bit = lax.axis_index("blk") % 2
    mine = lax.dynamic_index_in_dim(blocks, low_bit, 0, keepdims=False)
    theirs = lax.dynamic_index_in_dim(blocks, 1 - low_bit, 0, keepdims=False)
    chip = mine.astype(f32) + flipped(theirs, "blk", 1, blk_size).astype(f32)
    high, tp = lax.axis_index("blk") // 2, lax.axis_index("tp")
    total = None
    for bit in range(0, blk_size, 2):
        for shift in range(tp_size):
            piece = lax.dynamic_index_in_dim(chip, high ^ (bit // 2), 0, keepdims=False)
            piece = lax.dynamic_index_in_dim(piece, (tp + shift) % tp_size, 0, keepdims=False)
            if bit or shift:
                pairs = []
                for b in range(blk_size):
                    for t in range(tp_size):
                        pairs.append((b * tp_size + t, (b ^ bit) * tp_size + (t + shift) % tp_size))
                piece = lax.ppermute(piece.astype(bf16), ("blk", "tp"), pairs).astype(f32)
            total = piece if total is None else total + piece
    layer_out = total.astype(bf16)
    return (
        layer_out, query_grad, key_grad, value_grad, cross_grad, hk_grad, hv_grad, weight_grad,
    )


def on_device(*operands):
    grp, blk_size, tp_size = lax.axis_size("grp"), lax.axis_size("blk"), lax.axis_size("tp")
    row_count, width = operands[0].shape
    even = width % (grp * HD) == 0 and row_count % (16 * blk_size * tp_size) == 0
    pairs = blk_size % 2 == 0 and blk_size & (blk_size - 1) == 0
    fits = operands[8].shape[1] % (grp * (width // grp)) == 0
    if even and pairs and fits:
        return on_device_heads(grp, blk_size, tp_size, *operands)
    return on_device_tokens(*operands)


def solution(mesh):
    return jax.shard_map(
        on_device,
        mesh=mesh,
        in_specs=(
            P("grp", ("blk", "tp")),
            P("grp", ("blk", "tp")),
            P("grp", ("blk", "tp")),
            P("grp", ("blk", "tp")),
            P("grp", ("blk", "tp")),
            P("grp", ("blk", "tp")),
            P(),
            P(),
            P(("blk", "tp"), None),
            P("grp", ("blk", "tp")),
        ),
        out_specs=(
            P("grp", ("blk", "tp")),
            P("grp", ("blk", "tp")),
            P("grp", ("blk", "tp")),
            P("grp", ("blk", "tp")),
            P("grp", ("blk", "tp")),
            P("grp", ("blk", "tp")),
            P("grp", ("blk", "tp")),
            P(("blk", "tp"), "grp"),
        ),
        check_vma=False,
    )
```

```python
import functools

import jax
import jax.numpy as jnp
from jax import lax
from jax.experimental import pallas as pl
from jax.experimental.pallas import tpu as pltpu
from jax.sharding import PartitionSpec as P

HD = 128


def split_heads(matrix):
    return matrix.reshape(matrix.shape[0], matrix.shape[1] // HD, HD)


def merge_heads(tensor):
    return tensor.reshape(tensor.shape[0], tensor.shape[1] * tensor.shape[2])


def visible(query_frames, key_frames, key_masked, query_index, key_index):
    causal = key_frames[None, :] <= query_frames[:, None]
    open_key = (key_masked[None, :] == 0) | (key_index[None, :] == query_index[:, None])
    return causal & open_key


def scores_of(query_split, key_split, factor):
    return (
        jnp.einsum("qhd,khd->hqk", query_split, key_split, preferred_element_type=jnp.float32)
        * factor
    )


def softmax_parts(score):
    highest = jnp.max(score, axis=-1, keepdims=True)
    weights = jnp.exp(score - highest)
    summed = jnp.sum(weights, axis=-1, keepdims=True)
    return (weights / summed, highest[..., 0] + jnp.log(summed[..., 0]))


def key_side(dscore, prob_low, query_split, grad_split, factor):
    key_part = merge_heads(
        jnp.einsum("hqk,qhd->khd", dscore, query_split, preferred_element_type=jnp.float32) * factor
    )
    value_part = merge_heads(
        jnp.einsum("hqk,qhd->khd", prob_low, grad_split, preferred_element_type=jnp.float32)
    )
    return (key_part, value_part)


def on_device_tokens(
    queries,
    keys,
    values,
    cross_queries,
    history_keys,
    history_values,
    frame_ids,
    masked,
    out_weight,
    cotangent,
):
    row_count = queries.shape[0]
    factor = HD ** (-0.5)
    row_start = lax.axis_index("grp") * row_count
    query_index = row_start + jnp.arange(row_count, dtype=jnp.int32)
    every_key, every_value, past_keys, past_values = (
        lax.all_gather(keys, "grp", axis=0, tiled=True),
        lax.all_gather(values, "grp", axis=0, tiled=True),
        lax.all_gather(history_keys, "grp", axis=0, tiled=True),
        lax.all_gather(history_values, "grp", axis=0, tiled=True),
    )
    key_index = jnp.arange(every_key.shape[0], dtype=jnp.int32)
    query_frames = lax.dynamic_slice_in_dim(frame_ids, row_start, row_count)
    allowed = visible(query_frames, frame_ids, masked, query_index, key_index)
    query_split = split_heads(queries)
    cross_split = split_heads(cross_queries)
    key_split = split_heads(every_key)
    value_split = split_heads(every_value)
    memory_split = split_heads(past_keys)
    recall_split = split_heads(past_values)
    self_score = jnp.where(allowed[None], scores_of(query_split, key_split, factor), -jnp.inf)
    self_prob, self_log = softmax_parts(self_score)
    cross_prob, cross_log = softmax_parts(scores_of(cross_split, memory_split, factor))
    self_low = self_prob.astype(jnp.bfloat16)
    cross_low = cross_prob.astype(jnp.bfloat16)
    combined = jnp.einsum("hqk,khd->qhd", self_low, value_split, preferred_element_type=jnp.float32)
    combined = combined + jnp.einsum(
        "hqk,khd->qhd", cross_low, recall_split, preferred_element_type=jnp.float32
    )
    attended = merge_heads(combined).astype(jnp.bfloat16)
    head_terms = jnp.dot(attended, out_weight, preferred_element_type=jnp.float32)
    layer_out = lax.psum_scatter(head_terms, ("blk", "tp"), scatter_dimension=1, tiled=True).astype(
        jnp.bfloat16
    )
    arrived = lax.all_gather(cotangent, ("blk", "tp"), axis=1, tiled=True)
    grad_rows = lax.dot_general(
        arrived, out_weight, (((1,), (1,)), ((), ())), preferred_element_type=jnp.float32
    )
    product = lax.dot_general(
        attended, arrived, (((0,), (0,)), ((), ())), preferred_element_type=jnp.float32
    )
    grad_cols = product
    grad_rows, grad_cols = (grad_rows, grad_cols)
    weight_grad = lax.psum_scatter(
        grad_cols.astype(jnp.bfloat16), "grp", scatter_dimension=1, tiled=True
    ).astype(jnp.float32)
    grad_low = grad_rows.astype(jnp.bfloat16)
    grad_split = split_heads(grad_low)
    self_dprob = jnp.einsum(
        "qhd,khd->hqk", grad_split, value_split, preferred_element_type=jnp.float32
    )
    self_dot = jnp.sum(self_prob * self_dprob, axis=-1)
    self_dscore = (self_prob * (self_dprob - self_dot[..., None])).astype(jnp.bfloat16)
    cross_dprob = jnp.einsum(
        "qhd,khd->hqk", grad_split, recall_split, preferred_element_type=jnp.float32
    )
    cross_dot = jnp.sum(cross_prob * cross_dprob, axis=-1)
    cross_dscore = (cross_prob * (cross_dprob - cross_dot[..., None])).astype(jnp.bfloat16)
    query_grad = merge_heads(
        jnp.einsum("hqk,khd->qhd", self_dscore, key_split, preferred_element_type=jnp.float32)
        * factor
    ).astype(jnp.bfloat16)
    cross_grad = merge_heads(
        jnp.einsum("hqk,khd->qhd", cross_dscore, memory_split, preferred_element_type=jnp.float32)
        * factor
    ).astype(jnp.bfloat16)
    asked, asked_cross, asked_grad = (
        lax.all_gather(queries, "grp", axis=0, tiled=True),
        lax.all_gather(cross_queries, "grp", axis=0, tiled=True),
        lax.all_gather(grad_low, "grp", axis=0, tiled=True),
    )
    self_dots, cross_dots, self_logs, cross_logs = (
        lax.all_gather(self_dot, "grp", axis=1, tiled=True),
        lax.all_gather(cross_dot, "grp", axis=1, tiled=True),
        lax.all_gather(self_log, "grp", axis=1, tiled=True),
        lax.all_gather(cross_log, "grp", axis=1, tiled=True),
    )
    own_masked = lax.dynamic_slice_in_dim(masked, row_start, row_count)
    allowed_own = visible(frame_ids, query_frames, own_masked, key_index, query_index)
    asked_split = split_heads(asked)
    cross_every = split_heads(asked_cross)
    grad_every = split_heads(asked_grad)
    score_own = jnp.where(
        allowed_own[None], scores_of(asked_split, split_heads(keys), factor), -jnp.inf
    )
    prob_own = jnp.exp(score_own - self_logs[..., None])
    dprob_own = jnp.einsum(
        "qhd,khd->hqk", grad_every, split_heads(values), preferred_element_type=jnp.float32
    )
    dscore_own = (prob_own * (dprob_own - self_dots[..., None])).astype(jnp.bfloat16)
    key_part, value_part = key_side(
        dscore_own, prob_own.astype(jnp.bfloat16), asked_split, grad_every, factor
    )
    prob_past = jnp.exp(
        scores_of(cross_every, split_heads(history_keys), factor) - cross_logs[..., None]
    )
    dprob_past = jnp.einsum(
        "qhd,khd->hqk", grad_every, split_heads(history_values), preferred_element_type=jnp.float32
    )
    dscore_past = (prob_past * (dprob_past - cross_dots[..., None])).astype(jnp.bfloat16)
    memory_part, recall_part = key_side(
        dscore_past, prob_past.astype(jnp.bfloat16), cross_every, grad_every, factor
    )
    key_grad = key_part.astype(jnp.bfloat16)
    value_grad = value_part.astype(jnp.bfloat16)
    history_key_grad = memory_part.astype(jnp.bfloat16)
    history_value_grad = recall_part.astype(jnp.bfloat16)
    return (
        layer_out,
        query_grad,
        key_grad,
        value_grad,
        cross_grad,
        history_key_grad,
        history_value_grad,
        weight_grad,
    )


BF16, F32 = jnp.bfloat16, jnp.float32
ROWS_OF_TILE = 16


def lanes(index, size):
    return pl.ds(pl.multiple_of(index * size, 128), size)


def rows(start, size):
    return pl.ds(pl.multiple_of(start, ROWS_OF_TILE), size)


def contract(left, right, left_dim, right_dim):
    return lax.dot_general(
        left, right, (((left_dim,), (right_dim,)), ((), ())), preferred_element_type=F32
    )


def call(kernel, out_shapes, operands, scratch=(), flops=10**9, grant=24 << 20, space=None):
    whole = pl.BlockSpec(memory_space=pltpu.VMEM)
    return pl.pallas_call(
        kernel,
        out_shape=[jax.ShapeDtypeStruct(shape, dtype) for shape, dtype in out_shapes],
        in_specs=[pl.BlockSpec(memory_space=space) if space else whole] * len(operands),
        out_specs=[whole] * len(out_shapes),
        scratch_shapes=list(scratch),
        compiler_params=pltpu.CompilerParams(vmem_limit_bytes=grant),
        cost_estimate=pl.CostEstimate(flops=flops, bytes_accessed=1 << 20, transcendentals=0),
    )(*operands)


class Layout:
    def __init__(self, grp, blk, tp, row_count, past_count, width, cot_columns):
        self.grp, self.blk, self.tp = grp, blk, tp
        self.plane = blk * tp
        self.row_count, self.past_count, self.width = row_count, past_count, width
        self.own = width // grp
        self.lengths = [row_count] * 4 + [past_count] * 2
        self.starts = [sum(self.lengths[:i]) for i in range(6)]
        self.packed = sum(self.lengths)
        self.cot_columns = cot_columns
        self.cot_width = cot_columns * self.plane // grp
        self.part_rows = row_count // self.plane
        self.tiles = self.cot_width // self.own
        self.grad_rows = row_count + self.tiles * self.part_rows
        self.slots = [(bit, shift) for bit in range(0, blk, 2) for shift in range(tp)]

    def plane_pairs(self, bit, shift):
        return [
            (b * self.tp + t, (b ^ bit) * self.tp + (t + shift) % self.tp)
            for b in range(self.blk)
            for t in range(self.tp)
        ]

    def plane_rank(self, blk, bit, shift, back=False):
        tp = lax.axis_index("tp")
        step = self.tp - shift if back else shift
        return (blk ^ bit) * self.tp + (tp + step) % self.tp


def pack_kernel(lay, *refs):
    sources, cotangent, outs, held, sems, held_sem = (
        refs[:6], refs[6], refs[7:-3], refs[-3], refs[-2], refs[-1],
    )
    me = lax.axis_index("grp")
    copies = [pltpu.make_async_copy(cotangent, held, held_sem)]
    for s in range(lay.grp - 1, -1, -1):
        rank = (me + s) % lay.grp
        for i, (source, start, length) in enumerate(zip(sources, lay.starts, lay.lengths)):
            copy = pltpu.make_async_copy(
                source.at[:, lanes(rank, lay.own)],
                outs[s].at[start : start + length, :],
                sems.at[s, i],
            )
            copies.append(copy)
    for copy in copies[1:] + copies[:1]:
        copy.start()
    for copy in copies:
        copy.wait()


def load_kernel(weight, held, sems):
    count = sems.shape[0]
    step = weight.shape[0] // count
    copies = [
        pltpu.make_async_copy(
            weight.at[i * step : (i + 1) * step, :], held.at[i * step : (i + 1) * step, :], sems.at[i]
        )
        for i in range(count)
    ]
    for copy in copies:
        copy.start()
    for copy in copies:
        copy.wait()


def grad_kernel(lay, *refs):
    near = len(lay.slots)
    close, swapped, weight = refs[:near], refs[near], refs[near + 1]
    outs, part, grad = refs[near + 2 : -2], refs[-2], refs[-1]
    me, blk = lax.axis_index("grp"), lax.axis_index("blk")
    mine = rows(lay.part_rows * (blk * lay.tp + lax.axis_index("tp")), lay.part_rows)
    total = None
    for half in range(2):
        for i, (bit, shift) in enumerate(lay.slots):
            rank = lay.plane_rank(blk ^ half, bit, shift, back=True)
            block = close[i][...] if half == 0 else swapped[i]
            term = contract(block, weight[:, lanes(rank, lay.cot_columns)], 1, 1)
            total = term if total is None else total + term
            band = close[i][mine, :] if half == 0 else swapped[i, mine, :]
            part[:, lanes(rank, lay.cot_columns)] = band
    grad[...] = total.astype(BF16)
    for s, out in enumerate(outs):
        rank = (me + s) % lay.grp
        out[: lay.row_count, :] = grad[:, lanes(rank, lay.own)]
        for tile in range(lay.tiles):
            at = lay.row_count + tile * lay.part_rows
            out[at : at + lay.part_rows, :] = part[:, lanes(rank * lay.tiles + tile, lay.own)]


def head_columns(head):
    return slice(head * HD, (head + 1) * HD)


def joined(came, lay, index, head):
    start, length = lay.starts[index], lay.lengths[index]
    return jnp.concatenate([piece[start : start + length, head_columns(head)] for piece in came])


def piece_of(came, lay, index, slot, head):
    start, length = lay.starts[index], lay.lengths[index]
    return came[slot][start : start + length, head_columns(head)]


def open_entries(lay, slot, frames_row, frames_col, hidden):
    count = lay.grp * lay.row_count
    query_frames = frames_col[slot * lay.row_count : (slot + 1) * lay.row_count, :]
    causal = frames_row[...] <= query_frames
    shape = (lay.row_count, count)
    query = lax.broadcasted_iota(jnp.int32, shape, 0) + slot * lay.row_count
    key = lax.broadcasted_iota(jnp.int32, shape, 1)
    return causal & ((hidden[...] == 0) | (query == key))


def probabilities(query, key, limit):
    score = contract(query, key, 1, 1) * HD ** (-0.5)
    if limit is not None:
        score = jnp.where(limit, score, -jnp.inf)
    weights = jnp.exp(score - jnp.max(score, axis=-1, keepdims=True))
    return weights / jnp.sum(weights, axis=-1, keepdims=True)


def forward_kernel(lay, *refs):
    came, (frames_row, frames_col, hidden, attended) = refs[: lay.grp], refs[lay.grp :]
    me = lax.axis_index("grp")
    for head in range(lay.own // HD):
        key, value, past_key, past_value = [joined(came, lay, i, head) for i in (1, 2, 4, 5)]
        for slot in range(lay.grp):
            limit = open_entries(lay, slot, frames_row, frames_col, hidden)
            prob = probabilities(piece_of(came, lay, 0, slot, head), key, limit)
            past = probabilities(piece_of(came, lay, 3, slot, head), past_key, None)
            combined = contract(prob.astype(BF16), value, 1, 0)
            combined = combined + contract(past.astype(BF16), past_value, 1, 0)
            rank = (me + lay.grp - slot) % lay.grp
            attended[rows(rank * lay.row_count, lay.row_count), head_columns(head)] = (
                combined.astype(BF16)
            )


def backward_kernel(lay, *refs):
    n = lay.grp
    came, grads, (frames_row, frames_col, hidden) = refs[:n], refs[n : 2 * n], refs[2 * n : 2 * n + 3]
    outs, (low, slope, low_past, slope_past) = refs[2 * n + 3 : 3 * n + 3], refs[3 * n + 3 :]
    factor = HD ** (-0.5)
    for head in range(lay.own // HD):
        column = head_columns(head)
        key, value, past_key, past_value = [joined(came, lay, i, head) for i in (1, 2, 4, 5)]
        for slot in range(n):
            at = slice(slot * lay.row_count, (slot + 1) * lay.row_count)
            grad = grads[slot][: lay.row_count, column]
            for index, k, v, low_ref, slope_ref in (
                (0, key, value, low, slope),
                (3, past_key, past_value, low_past, slope_past),
            ):
                limit = None
                if index == 0:
                    limit = open_entries(lay, slot, frames_row, frames_col, hidden)
                prob = probabilities(piece_of(came, lay, index, slot, head), k, limit)
                dprob = contract(grad, v, 1, 1)
                dot = jnp.sum(prob * dprob, axis=-1, keepdims=True)
                dscore = (prob * (dprob - dot)).astype(BF16)
                low_ref[at, :] = prob.astype(BF16)
                slope_ref[at, :] = dscore
                start = lay.starts[index]
                outs[slot][start : start + lay.row_count, column] = (
                    contract(dscore, k, 1, 0) * factor
                ).astype(BF16)
        grad = jnp.concatenate([piece[: lay.row_count, column] for piece in grads])
        query, cross = joined(came, lay, 0, head), joined(came, lay, 3, head)
        for index, result in (
            (1, contract(slope[...], query, 0, 0) * factor),
            (2, contract(low[...], grad, 0, 0)),
            (4, contract(slope_past[...], cross, 0, 0) * factor),
            (5, contract(low_past[...], grad, 0, 0)),
        ):
            start, length = lay.starts[index], lay.lengths[index]
            for slot in range(n):
                outs[slot][start : start + length, column] = result[
                    slot * length : (slot + 1) * length
                ].astype(BF16)


def unpack_kernel(lay, *refs):
    back, outs = refs[: lay.grp], refs[lay.grp :]
    me = lax.axis_index("grp")
    for s, piece in enumerate(back):
        rank = (me + s) % lay.grp
        for out, start, length in zip(outs, lay.starts, lay.lengths):
            out[:, lanes(rank, lay.own)] = piece[start : start + length, :]


def weight_kernel(lay, *refs):
    near = len(lay.slots)
    spread, close, swapped = refs[: lay.grp], refs[lay.grp : lay.grp + near], refs[lay.grp + near]
    out, cot = refs[lay.grp + near + 1 :]
    me, blk = lax.axis_index("grp"), lax.axis_index("blk")
    for half in range(2):
        for i, (bit, shift) in enumerate(lay.slots):
            plane = lay.plane_rank(blk ^ half, bit, shift, back=True)
            for s in range(lay.grp):
                rank = (me + lay.grp - s) % lay.grp
                to = rows(rank * lay.row_count + plane * lay.part_rows, lay.part_rows)
                for tile in range(lay.tiles):
                    at = (s * lay.tiles + tile) * lay.part_rows
                    at = slice(at, at + lay.part_rows)
                    band = close[i][at, :] if half == 0 else swapped[i, at, :]
                    cot[to, tile * lay.own : (tile + 1) * lay.own] = band
    for s in range(lay.grp):
        rank = (me + lay.grp - s) % lay.grp
        out[rows(rank * lay.own, lay.own), :] = contract(spread[s][...], cot[...], 0, 0)


def terms_kernel(lay, *refs):
    spread, weight, mine, theirs, both = refs[: lay.grp], refs[-4], refs[-3], refs[-2], refs[-1]
    me, blk = lax.axis_index("grp"), lax.axis_index("blk")
    for s in range(lay.grp):
        rank = (me + lay.grp - s) % lay.grp
        both[:, lanes(rank, lay.own)] = spread[s][rows(me * lay.row_count, lay.row_count), :]
    left = both[...]
    for half, out in ((1, theirs), (0, mine)):
        for i, (bit, shift) in enumerate(lay.slots):
            rank = lay.plane_rank(blk ^ half, bit, shift)
            term = contract(left, weight[:, lanes(rank, lay.cot_columns)], 1, 0)
            out[i] = term.astype(out.dtype)


def shifted(piece, shift, size):
    return lax.ppermute(piece, "grp", [(i, (i + shift) % size) for i in range(size)])


def in_hbm(array):
    return pltpu.with_memory_space_constraint(array, pltpu.HBM)


def swap_cores(lay, piece):
    return lax.ppermute(piece, "blk", [(i, i ^ 1) for i in range(lay.blk)])


def to_slot(lay, piece, i):
    return lax.ppermute(piece, ("blk", "tp"), lay.plane_pairs(*lay.slots[i]))


def plane_gather(lay, piece):
    close = [piece] + [to_slot(lay, piece, i) for i in range(1, len(lay.slots))]
    return close, swap_cores(lay, jnp.stack(close))


def on_device_heads(
    lay, queries, keys, values, cross_queries, history_keys, history_values,
    frame_ids, masked, out_weight, cotangent,
):
    n, row_count, own = lay.grp, lay.row_count, lay.own
    me = lax.axis_index("grp")
    sources = [queries, keys, values, cross_queries, history_keys, history_values]
    packed = call(
        functools.partial(pack_kernel, lay),
        [((lay.packed, own), BF16)] * n + [(cotangent.shape, BF16)],
        [in_hbm(source) for source in sources + [cotangent]],
        [pltpu.SemaphoreType.DMA((n, 6)), pltpu.SemaphoreType.DMA],
        flops=10**8,
        space=pltpu.HBM,
    )
    cotangent = packed[n]
    out_weight = call(
        load_kernel,
        [(out_weight.shape, BF16)],
        [in_hbm(out_weight)],
        [pltpu.SemaphoreType.DMA((4,))],
        space=pltpu.HBM,
    )[0]
    came = [packed[0]] + [shifted(packed[s], s, n) for s in range(1, n)]

    close, swapped = plane_gather(lay, cotangent)
    outgoing = call(
        functools.partial(grad_kernel, lay),
        [((lay.grad_rows, own), BF16)] * n,
        close + [swapped, out_weight],
        [
            pltpu.VMEM((lay.part_rows, lay.cot_columns * lay.plane), BF16),
            pltpu.VMEM((row_count, lay.width), BF16),
        ],
    )
    grads = [outgoing[0]] + [shifted(outgoing[s], s, n) for s in range(1, n)]

    def by_slot(vector):
        parts = vector.reshape(n, row_count)[::-1]
        parts = jnp.concatenate([parts, parts])
        return lax.dynamic_slice_in_dim(parts, n - 1 - me, n, axis=0).reshape(-1)

    frames, hidden = by_slot(frame_ids), by_slot(masked)
    marks = [frames[None, :], frames[:, None], hidden[None, :]]
    attended = call(
        functools.partial(forward_kernel, lay), [((n * row_count, own), BF16)], came + marks
    )[0]
    spread = [attended] + [shifted(attended, s, n) for s in range(1, n)]

    count, past = n * row_count, n * lay.past_count
    results = call(
        functools.partial(backward_kernel, lay),
        [((lay.packed, own), BF16)] * n,
        came + grads + marks,
        [pltpu.VMEM((count, size), BF16) for size in (count, count, past, past)],
        flops=2 * 10**9,
    )
    back = [results[0]] + [shifted(results[s], -s, n) for s in range(1, n)]
    restored = call(
        functools.partial(unpack_kernel, lay),
        [(source.shape, BF16) for source in sources],
        back,
        flops=10**8,
    )

    cot_piece = jnp.concatenate([piece[row_count:] for piece in grads])
    cot_close, cot_swapped = plane_gather(lay, cot_piece)
    weight_grad = call(
        functools.partial(weight_kernel, lay),
        [((lay.width, lay.cot_width), F32)],
        spread + cot_close + [cot_swapped],
        [pltpu.VMEM((count, lay.cot_width), BF16)],
    )[0]

    slots = len(lay.slots)
    shape = (slots, row_count, lay.cot_columns)
    mine, theirs = call(
        functools.partial(terms_kernel, lay),
        [(shape, F32), (shape, BF16)],
        spread + [out_weight],
        [pltpu.VMEM((row_count, lay.width), BF16)],
    )
    chip = mine + swap_cores(lay, theirs).astype(F32)
    total = chip[0]
    for i in range(1, slots):
        total = total + to_slot(lay, chip[i].astype(BF16), i).astype(F32)
    return (total.astype(BF16), *restored, weight_grad)


def on_device(*operands):
    grp, blk, tp = lax.axis_size("grp"), lax.axis_size("blk"), lax.axis_size("tp")
    row_count, width = operands[0].shape
    cot_columns = operands[9].shape[1]
    plane = blk * tp
    fits = (
        width % (grp * HD) == 0
        and row_count % (ROWS_OF_TILE * plane) == 0
        and blk & (blk - 1) == 0
        and blk > 1
        and cot_columns % 128 == 0
        and (cot_columns * plane) % (width // grp * grp) == 0
    )
    if fits:
        lay = Layout(grp, blk, tp, row_count, operands[4].shape[0], width, cot_columns)
        return on_device_heads(lay, *operands)
    return on_device_tokens(*operands)


def solution(mesh):
    return jax.shard_map(
        on_device,
        mesh=mesh,
        in_specs=(
            P("grp", ("blk", "tp")),
            P("grp", ("blk", "tp")),
            P("grp", ("blk", "tp")),
            P("grp", ("blk", "tp")),
            P("grp", ("blk", "tp")),
            P("grp", ("blk", "tp")),
            P(),
            P(),
            P(("blk", "tp"), None),
            P("grp", ("blk", "tp")),
        ),
        out_specs=(
            P("grp", ("blk", "tp")),
            P("grp", ("blk", "tp")),
            P("grp", ("blk", "tp")),
            P("grp", ("blk", "tp")),
            P("grp", ("blk", "tp")),
            P("grp", ("blk", "tp")),
            P("grp", ("blk", "tp")),
            P(("blk", "tp"), "grp"),
        ),
        check_vma=False,
    )
```

```python
import functools

import jax
import jax.numpy as jnp
from jax import lax
from jax.experimental import pallas as pl
from jax.experimental.pallas import tpu as pltpu
from jax.sharding import PartitionSpec as P

HD = 128


def split_heads(matrix):
    return matrix.reshape(matrix.shape[0], matrix.shape[1] // HD, HD)


def merge_heads(tensor):
    return tensor.reshape(tensor.shape[0], tensor.shape[1] * tensor.shape[2])


def visible(query_frames, key_frames, key_masked, query_index, key_index):
    causal = key_frames[None, :] <= query_frames[:, None]
    open_key = (key_masked[None, :] == 0) | (key_index[None, :] == query_index[:, None])
    return causal & open_key


def scores_of(query_split, key_split, factor):
    return (
        jnp.einsum("qhd,khd->hqk", query_split, key_split, preferred_element_type=jnp.float32)
        * factor
    )


def softmax_parts(score):
    highest = jnp.max(score, axis=-1, keepdims=True)
    weights = jnp.exp(score - highest)
    summed = jnp.sum(weights, axis=-1, keepdims=True)
    return (weights / summed, highest[..., 0] + jnp.log(summed[..., 0]))


def key_side(dscore, prob_low, query_split, grad_split, factor):
    key_part = merge_heads(
        jnp.einsum("hqk,qhd->khd", dscore, query_split, preferred_element_type=jnp.float32) * factor
    )
    value_part = merge_heads(
        jnp.einsum("hqk,qhd->khd", prob_low, grad_split, preferred_element_type=jnp.float32)
    )
    return (key_part, value_part)


def on_device_tokens(
    queries,
    keys,
    values,
    cross_queries,
    history_keys,
    history_values,
    frame_ids,
    masked,
    out_weight,
    cotangent,
):
    row_count = queries.shape[0]
    factor = HD ** (-0.5)
    row_start = lax.axis_index("grp") * row_count
    query_index = row_start + jnp.arange(row_count, dtype=jnp.int32)
    every_key, every_value, past_keys, past_values = (
        lax.all_gather(keys, "grp", axis=0, tiled=True),
        lax.all_gather(values, "grp", axis=0, tiled=True),
        lax.all_gather(history_keys, "grp", axis=0, tiled=True),
        lax.all_gather(history_values, "grp", axis=0, tiled=True),
    )
    key_index = jnp.arange(every_key.shape[0], dtype=jnp.int32)
    query_frames = lax.dynamic_slice_in_dim(frame_ids, row_start, row_count)
    allowed = visible(query_frames, frame_ids, masked, query_index, key_index)
    query_split = split_heads(queries)
    cross_split = split_heads(cross_queries)
    key_split = split_heads(every_key)
    value_split = split_heads(every_value)
    memory_split = split_heads(past_keys)
    recall_split = split_heads(past_values)
    self_score = jnp.where(allowed[None], scores_of(query_split, key_split, factor), -jnp.inf)
    self_prob, self_log = softmax_parts(self_score)
    cross_prob, cross_log = softmax_parts(scores_of(cross_split, memory_split, factor))
    self_low = self_prob.astype(jnp.bfloat16)
    cross_low = cross_prob.astype(jnp.bfloat16)
    combined = jnp.einsum("hqk,khd->qhd", self_low, value_split, preferred_element_type=jnp.float32)
    combined = combined + jnp.einsum(
        "hqk,khd->qhd", cross_low, recall_split, preferred_element_type=jnp.float32
    )
    attended = merge_heads(combined).astype(jnp.bfloat16)
    head_terms = jnp.dot(attended, out_weight, preferred_element_type=jnp.float32)
    layer_out = lax.psum_scatter(head_terms, ("blk", "tp"), scatter_dimension=1, tiled=True).astype(
        jnp.bfloat16
    )
    arrived = lax.all_gather(cotangent, ("blk", "tp"), axis=1, tiled=True)
    grad_rows = lax.dot_general(
        arrived, out_weight, (((1,), (1,)), ((), ())), preferred_element_type=jnp.float32
    )
    product = lax.dot_general(
        attended, arrived, (((0,), (0,)), ((), ())), preferred_element_type=jnp.float32
    )
    grad_cols = product
    grad_rows, grad_cols = (grad_rows, grad_cols)
    weight_grad = lax.psum_scatter(
        grad_cols.astype(jnp.bfloat16), "grp", scatter_dimension=1, tiled=True
    ).astype(jnp.float32)
    grad_low = grad_rows.astype(jnp.bfloat16)
    grad_split = split_heads(grad_low)
    self_dprob = jnp.einsum(
        "qhd,khd->hqk", grad_split, value_split, preferred_element_type=jnp.float32
    )
    self_dot = jnp.sum(self_prob * self_dprob, axis=-1)
    self_dscore = (self_prob * (self_dprob - self_dot[..., None])).astype(jnp.bfloat16)
    cross_dprob = jnp.einsum(
        "qhd,khd->hqk", grad_split, recall_split, preferred_element_type=jnp.float32
    )
    cross_dot = jnp.sum(cross_prob * cross_dprob, axis=-1)
    cross_dscore = (cross_prob * (cross_dprob - cross_dot[..., None])).astype(jnp.bfloat16)
    query_grad = merge_heads(
        jnp.einsum("hqk,khd->qhd", self_dscore, key_split, preferred_element_type=jnp.float32)
        * factor
    ).astype(jnp.bfloat16)
    cross_grad = merge_heads(
        jnp.einsum("hqk,khd->qhd", cross_dscore, memory_split, preferred_element_type=jnp.float32)
        * factor
    ).astype(jnp.bfloat16)
    asked, asked_cross, asked_grad = (
        lax.all_gather(queries, "grp", axis=0, tiled=True),
        lax.all_gather(cross_queries, "grp", axis=0, tiled=True),
        lax.all_gather(grad_low, "grp", axis=0, tiled=True),
    )
    self_dots, cross_dots, self_logs, cross_logs = (
        lax.all_gather(self_dot, "grp", axis=1, tiled=True),
        lax.all_gather(cross_dot, "grp", axis=1, tiled=True),
        lax.all_gather(self_log, "grp", axis=1, tiled=True),
        lax.all_gather(cross_log, "grp", axis=1, tiled=True),
    )
    own_masked = lax.dynamic_slice_in_dim(masked, row_start, row_count)
    allowed_own = visible(frame_ids, query_frames, own_masked, key_index, query_index)
    asked_split = split_heads(asked)
    cross_every = split_heads(asked_cross)
    grad_every = split_heads(asked_grad)
    score_own = jnp.where(
        allowed_own[None], scores_of(asked_split, split_heads(keys), factor), -jnp.inf
    )
    prob_own = jnp.exp(score_own - self_logs[..., None])
    dprob_own = jnp.einsum(
        "qhd,khd->hqk", grad_every, split_heads(values), preferred_element_type=jnp.float32
    )
    dscore_own = (prob_own * (dprob_own - self_dots[..., None])).astype(jnp.bfloat16)
    key_part, value_part = key_side(
        dscore_own, prob_own.astype(jnp.bfloat16), asked_split, grad_every, factor
    )
    prob_past = jnp.exp(
        scores_of(cross_every, split_heads(history_keys), factor) - cross_logs[..., None]
    )
    dprob_past = jnp.einsum(
        "qhd,khd->hqk", grad_every, split_heads(history_values), preferred_element_type=jnp.float32
    )
    dscore_past = (prob_past * (dprob_past - cross_dots[..., None])).astype(jnp.bfloat16)
    memory_part, recall_part = key_side(
        dscore_past, prob_past.astype(jnp.bfloat16), cross_every, grad_every, factor
    )
    key_grad = key_part.astype(jnp.bfloat16)
    value_grad = value_part.astype(jnp.bfloat16)
    history_key_grad = memory_part.astype(jnp.bfloat16)
    history_value_grad = recall_part.astype(jnp.bfloat16)
    return (
        layer_out,
        query_grad,
        key_grad,
        value_grad,
        cross_grad,
        history_key_grad,
        history_value_grad,
        weight_grad,
    )


BF16, F32 = jnp.bfloat16, jnp.float32
ROWS_OF_TILE = 16


def lanes(index, size):
    return pl.ds(pl.multiple_of(index * size, 128), size)


def rows(start, size):
    return pl.ds(pl.multiple_of(start, ROWS_OF_TILE), size)


def contract(left, right, left_dim, right_dim):
    return lax.dot_general(
        left, right, (((left_dim,), (right_dim,)), ((), ())), preferred_element_type=F32
    )


def call(kernel, out_shapes, operands, scratch=(), flops=10**9, grant=16 << 20, all_in_hbm=False, last_in_hbm=False):
    whole, far = pl.BlockSpec(memory_space=pltpu.VMEM), pl.BlockSpec(memory_space=pltpu.HBM)
    specs = [far if all_in_hbm else whole] * len(operands)
    if last_in_hbm:
        specs[-1] = far
    return pl.pallas_call(
        kernel,
        out_shape=[jax.ShapeDtypeStruct(shape, dtype) for shape, dtype in out_shapes],
        in_specs=specs,
        out_specs=[whole] * len(out_shapes),
        scratch_shapes=list(scratch),
        compiler_params=pltpu.CompilerParams(vmem_limit_bytes=grant),
        cost_estimate=pl.CostEstimate(flops=flops, bytes_accessed=1 << 20, transcendentals=0),
    )(*operands)


class Layout:
    def __init__(self, grp, blk, tp, row_count, past_count, width, cot_columns):
        self.grp, self.blk, self.tp = grp, blk, tp
        self.plane = blk * tp
        self.row_count, self.past_count, self.width = row_count, past_count, width
        self.own = width // grp
        self.lengths = [row_count] * 4 + [past_count] * 2
        self.starts = [sum(self.lengths[:i]) for i in range(6)]
        self.packed = sum(self.lengths)
        self.cot_columns = cot_columns
        self.cot_width = cot_columns * self.plane // grp
        self.part_rows = row_count // self.plane
        self.tiles = self.cot_width // self.own
        self.grad_rows = row_count + self.tiles * self.part_rows
        self.relay = 2 if grp == 4 else 0
        self.slots = [(bit, shift) for bit in range(0, blk, 2) for shift in range(tp)]

    def plane_pairs(self, bit, shift):
        return [
            (b * self.tp + t, (b ^ bit) * self.tp + (t + shift) % self.tp)
            for b in range(self.blk)
            for t in range(self.tp)
        ]

    def plane_rank(self, blk, bit, shift, back=False):
        tp = lax.axis_index("tp")
        step = self.tp - shift if back else shift
        return (blk ^ bit) * self.tp + (tp + step) % self.tp


def pack_kernel(lay, *refs):
    sources, cotangent, outs, held, sems, held_sem = (
        refs[:6], refs[6], refs[7:-3], refs[-3], refs[-2], refs[-1],
    )
    me = lax.axis_index("grp")
    copies = [pltpu.make_async_copy(cotangent, held, held_sem)]
    for s in range(lay.grp - 1, -1, -1):
        rank = me ^ s
        for i, (source, start, length) in enumerate(zip(sources, lay.starts, lay.lengths)):
            copy = pltpu.make_async_copy(
                source.at[:, lanes(rank, lay.own)],
                outs[s].at[start : start + length, :],
                sems.at[s, i],
            )
            copies.append(copy)
    for copy in copies[1:] + copies[:1]:
        copy.start()
    for copy in copies:
        copy.wait()


def weight_columns(lay, weight, held, sems, ranks):
    copies = [
        pltpu.make_async_copy(weight.at[:, lanes(rank, lay.cot_columns)], held.at[i], sems.at[i])
        for i, rank in enumerate(ranks)
    ]
    for copy in copies:
        copy.start()
    return copies


def stack_kernel(*refs):
    for i, piece in enumerate(refs[:-1]):
        refs[-1][i] = piece[...]


def finish_kernel(own, *refs):
    total = own[...]
    for piece in refs[:-1]:
        total = total + piece[...].astype(F32)
    refs[-1][...] = total.astype(BF16)


def near_kernel(lay, *refs):
    near = len(lay.slots)
    close, weight, total_ref, part, far, held, sems, far_sems = refs[:near], *refs[near:]
    blk = lax.axis_index("blk")
    mine = rows(lay.part_rows * (blk * lay.tp + lax.axis_index("tp")), lay.part_rows)
    ranks = [lay.plane_rank(blk, bit, shift, back=True) for bit, shift in lay.slots]
    copies = weight_columns(lay, weight, held, sems, ranks)
    others = [lay.plane_rank(blk ^ 1, bit, shift, back=True) for bit, shift in lay.slots]
    far_copies = weight_columns(lay, weight, far, far_sems, others)
    total = None
    for i, rank in enumerate(ranks):
        part[:, lanes(rank, lay.cot_columns)] = close[i][mine, :]
        copies[i].wait()
        term = contract(close[i][...], held[i], 1, 1)
        total = term if total is None else total + term
    total_ref[...] = total
    for copy in far_copies:
        copy.wait()


def grad_kernel(lay, *refs):
    swapped, total_ref, near_part, weight = refs[:4]
    outs, (part, grad) = refs[4:-2], refs[-2:]
    me, blk = lax.axis_index("grp"), lax.axis_index("blk")
    mine = rows(lay.part_rows * (blk * lay.tp + lax.axis_index("tp")), lay.part_rows)
    ranks = [lay.plane_rank(blk ^ 1, bit, shift, back=True) for bit, shift in lay.slots]
    part[...] = near_part[...]
    for i, rank in enumerate(ranks):
        part[:, lanes(rank, lay.cot_columns)] = swapped[i, mine, :]
    total = total_ref[...]
    for i in range(len(ranks)):
        total = total + contract(swapped[i], weight[i], 1, 1)
    grad[...] = total.astype(BF16)
    for s, out in enumerate(outs):
        rank = me ^ s
        out[: lay.row_count, :] = grad[:, lanes(rank, lay.own)]
        for tile in range(lay.tiles):
            at = lay.row_count + tile * lay.part_rows
            out[at : at + lay.part_rows, :] = part[:, lanes(rank * lay.tiles + tile, lay.own)]


def head_columns(head):
    return slice(head * HD, (head + 1) * HD)


def joined(came, lay, index, head):
    start, length = lay.starts[index], lay.lengths[index]
    return jnp.concatenate([piece[start : start + length, head_columns(head)] for piece in came])


def piece_of(came, lay, index, slot, head):
    start, length = lay.starts[index], lay.lengths[index]
    return came[slot][start : start + length, head_columns(head)]


def open_entries(lay, slot, frames_row, frames_col, hidden):
    me = lax.axis_index("grp")
    count = lay.grp * lay.row_count

    def by_slot(ref):
        return jnp.concatenate([ref[:, lanes(me ^ s, lay.row_count)] for s in range(lay.grp)], axis=1)

    query_frames = frames_col[rows((me ^ slot) * lay.row_count, lay.row_count), :]
    causal = by_slot(frames_row) <= query_frames
    shape = (lay.row_count, count)
    query = lax.broadcasted_iota(jnp.int32, shape, 0) + slot * lay.row_count
    key = lax.broadcasted_iota(jnp.int32, shape, 1)
    return causal & ((by_slot(hidden) == 0) | (query == key))


def probabilities(query, key, limit):
    score = contract(query, key, 1, 1) * HD ** (-0.5)
    if limit is not None:
        score = jnp.where(limit, score, -jnp.inf)
    weights = jnp.exp(score - jnp.max(score, axis=-1, keepdims=True))
    return weights / jnp.sum(weights, axis=-1, keepdims=True)


def forward_kernel(lay, *refs):
    came, (frames_row, frames_col, hidden, attended) = refs[: lay.grp], refs[lay.grp :]
    me = lax.axis_index("grp")
    for head in range(lay.own // HD):
        key, value, past_key, past_value = [joined(came, lay, i, head) for i in (1, 2, 4, 5)]
        for slot in range(lay.grp):
            limit = open_entries(lay, slot, frames_row, frames_col, hidden)
            prob = probabilities(piece_of(came, lay, 0, slot, head), key, limit)
            past = probabilities(piece_of(came, lay, 3, slot, head), past_key, None)
            combined = contract(prob.astype(BF16), value, 1, 0)
            combined = combined + contract(past.astype(BF16), past_value, 1, 0)
            rank = me ^ slot
            attended[rows(rank * lay.row_count, lay.row_count), head_columns(head)] = (
                combined.astype(BF16)
            )


def backward_kernel(lay, *refs):
    n = lay.grp
    came, grads, (frames_row, frames_col, hidden) = refs[:n], refs[n : 2 * n], refs[2 * n : 2 * n + 3]
    outs, (low, slope, low_past, slope_past) = refs[2 * n + 3 : 3 * n + 3], refs[3 * n + 3 :]
    factor = HD ** (-0.5)
    for head in range(lay.own // HD):
        column = head_columns(head)
        key, value, past_key, past_value = [joined(came, lay, i, head) for i in (1, 2, 4, 5)]
        for slot in range(n):
            at = slice(slot * lay.row_count, (slot + 1) * lay.row_count)
            grad = grads[slot][: lay.row_count, column]
            for index, k, v, low_ref, slope_ref in (
                (0, key, value, low, slope),
                (3, past_key, past_value, low_past, slope_past),
            ):
                limit = None
                if index == 0:
                    limit = open_entries(lay, slot, frames_row, frames_col, hidden)
                prob = probabilities(piece_of(came, lay, index, slot, head), k, limit)
                dprob = contract(grad, v, 1, 1)
                dot = jnp.sum(prob * dprob, axis=-1, keepdims=True)
                dscore = (prob * (dprob - dot)).astype(BF16)
                low_ref[at, :] = prob.astype(BF16)
                slope_ref[at, :] = dscore
                start = lay.starts[index]
                outs[slot][start : start + lay.row_count, column] = (
                    contract(dscore, k, 1, 0) * factor
                ).astype(BF16)
        grad = jnp.concatenate([piece[: lay.row_count, column] for piece in grads])
        query, cross = joined(came, lay, 0, head), joined(came, lay, 3, head)
        for index, result in (
            (1, contract(slope[...], query, 0, 0) * factor),
            (2, contract(low[...], grad, 0, 0)),
            (4, contract(slope_past[...], cross, 0, 0) * factor),
            (5, contract(low_past[...], grad, 0, 0)),
        ):
            start, length = lay.starts[index], lay.lengths[index]
            for slot in range(n):
                outs[slot][start : start + length, column] = result[
                    slot * length : (slot + 1) * length
                ].astype(BF16)


def unpack_kernel(lay, *refs):
    back, outs = refs[: lay.grp], refs[lay.grp :]
    me = lax.axis_index("grp")
    for s, piece in enumerate(back):
        rank = me ^ s
        for out, start, length in zip(outs, lay.starts, lay.lengths):
            out[:, lanes(rank, lay.own)] = piece[start : start + length, :]


def weight_kernel(lay, *refs):
    near = len(lay.slots)
    spread, close, swapped = refs[: lay.grp], refs[lay.grp : lay.grp + near], refs[lay.grp + near]
    out, cot = refs[lay.grp + near + 1 :]
    me, blk = lax.axis_index("grp"), lax.axis_index("blk")
    for half in range(2):
        for i, (bit, shift) in enumerate(lay.slots):
            plane = lay.plane_rank(blk ^ half, bit, shift, back=True)
            for s in range(lay.grp):
                rank = me ^ s
                to = rows(rank * lay.row_count + plane * lay.part_rows, lay.part_rows)
                for tile in range(lay.tiles):
                    at = (s * lay.tiles + tile) * lay.part_rows
                    at = slice(at, at + lay.part_rows)
                    band = close[i][at, :] if half == 0 else swapped[i, at, :]
                    cot[to, tile * lay.own : (tile + 1) * lay.own] = band
    for s in range(lay.grp):
        rank = me ^ s
        out[rows(rank * lay.own, lay.own), :] = contract(spread[s][...], cot[...], 0, 0)


def terms_kernel(lay, *refs):
    spread, (weight, out, both) = refs[: lay.grp], refs[lay.grp :]
    me = lax.axis_index("grp")
    for s in range(lay.grp):
        columns = lanes(me ^ s, lay.own)
        both[:, columns] = spread[s][rows(me * lay.row_count, lay.row_count), :]
    left = both[...]
    for i, (bit, shift) in enumerate(lay.slots):
        at = lay.slots.index((bit, (lay.tp - shift) % lay.tp))
        out[i] = contract(left, weight[at], 1, 0).astype(out.dtype)


def exchanged(piece, step, size):
    return lax.ppermute(piece, "grp", [(i, i ^ step) for i in range(size)])


def in_hbm(array):
    return pltpu.with_memory_space_constraint(array, pltpu.HBM)


def swap_cores(lay, piece):
    return lax.ppermute(piece, "blk", [(i, i ^ 1) for i in range(lay.blk)])


def to_slot(lay, piece, i):
    return lax.ppermute(piece, ("blk", "tp"), lay.plane_pairs(*lay.slots[i]))


def plane_gather(lay, piece, held):
    close = [held] + [to_slot(lay, piece, i) for i in range(1, len(lay.slots))]
    shape = (len(close),) + piece.shape
    both = call(stack_kernel, [(shape, BF16)], close, flops=10**7)[0]
    return close, swap_cores(lay, both)


def on_device_heads(
    lay, queries, keys, values, cross_queries, history_keys, history_values,
    frame_ids, masked, out_weight, cotangent,
):
    n, row_count, own = lay.grp, lay.row_count, lay.own
    sources = [queries, keys, values, cross_queries, history_keys, history_values]
    packed = call(
        functools.partial(pack_kernel, lay),
        [((lay.packed, own), BF16)] * n + [(cotangent.shape, BF16)],
        [in_hbm(source) for source in sources + [cotangent]],
        [pltpu.SemaphoreType.DMA((n, 6)), pltpu.SemaphoreType.DMA],
        flops=10**8,
        all_in_hbm=True,
    )
    out_weight = in_hbm(out_weight)
    came = [packed[0]] + [exchanged(packed[s], s, n) for s in range(1, n)]

    close, swapped = plane_gather(lay, cotangent, packed[n])
    slots = len(lay.slots)
    part_shape = (lay.part_rows, lay.cot_columns * lay.plane)
    half_shape = (slots, lay.width, lay.cot_columns)
    total, part, far_weight, near_weight = call(
        functools.partial(near_kernel, lay),
        [((row_count, lay.width), F32), (part_shape, BF16), (half_shape, BF16), (half_shape, BF16)],
        close + [out_weight],
        [pltpu.SemaphoreType.DMA((slots,))] * 2,
        last_in_hbm=True,
    )
    outgoing = call(
        functools.partial(grad_kernel, lay),
        [((lay.grad_rows, own), BF16)] * n,
        [swapped, total, part, far_weight],
        [pltpu.VMEM(part_shape, BF16), pltpu.VMEM((row_count, lay.width), BF16)],
    )
    grads = [outgoing[0]] + [exchanged(outgoing[s], s, n) for s in range(1, n)]

    marks = [frame_ids[None, :], frame_ids[:, None], masked[None, :]]
    attended = call(
        functools.partial(forward_kernel, lay), [((n * row_count, own), BF16)], came + marks
    )[0]
    spread = [attended] + [exchanged(attended, s, n) for s in range(1, n) if s != lay.relay]
    if lay.relay:
        spread.insert(lay.relay, exchanged(spread[-1], lay.relay ^ (n - 1), n))

    count, past = n * row_count, n * lay.past_count
    results = call(
        functools.partial(backward_kernel, lay),
        [((lay.packed, own), BF16)] * n,
        came + grads + marks,
        [pltpu.VMEM((count, size), BF16) for size in (count, count, past, past)],
        flops=2 * 10**9,
    )
    back = [results[0]] + [exchanged(results[s], s, n) for s in range(1, n)]
    restored = call(
        functools.partial(unpack_kernel, lay),
        [(source.shape, BF16) for source in sources],
        back,
        flops=10**8,
    )

    cot_piece = jnp.concatenate([piece[row_count:] for piece in grads])
    cot_close, cot_swapped = plane_gather(lay, cot_piece, cot_piece)
    weight_grad = call(
        functools.partial(weight_kernel, lay),
        [((lay.width, lay.cot_width), F32)],
        spread + cot_close + [cot_swapped],
        [pltpu.VMEM((count, lay.cot_width), BF16)],
    )[0]

    shape = (slots, row_count, lay.cot_columns)
    theirs, mine = [
        call(
            functools.partial(terms_kernel, lay),
            [(shape, dtype)],
            spread + [half],
            [pltpu.VMEM((row_count, lay.width), BF16)],
        )[0]
        for half, dtype in ((far_weight, BF16), (near_weight, F32))
    ]
    chip = mine + swap_cores(lay, theirs).astype(F32)
    parts = [to_slot(lay, chip[i].astype(BF16), i) for i in range(1, slots)]
    layer_out = call(finish_kernel, [(cotangent.shape, BF16)], [chip[0]] + parts, flops=10**7)[0]
    return (layer_out, *restored, weight_grad)


def on_device(*operands):
    grp, blk, tp = lax.axis_size("grp"), lax.axis_size("blk"), lax.axis_size("tp")
    row_count, width = operands[0].shape
    cot_columns = operands[9].shape[1]
    plane = blk * tp
    fits = (
        width % (grp * HD) == 0
        and row_count % (ROWS_OF_TILE * plane) == 0
        and grp & (grp - 1) == 0
        and blk & (blk - 1) == 0
        and blk > 1
        and cot_columns % 128 == 0
        and (cot_columns * plane) % (width // grp * grp) == 0
    )
    if fits:
        lay = Layout(grp, blk, tp, row_count, operands[4].shape[0], width, cot_columns)
        return on_device_heads(lay, *operands)
    return on_device_tokens(*operands)


def solution(mesh):
    return jax.shard_map(
        on_device,
        mesh=mesh,
        in_specs=(
            P("grp", ("blk", "tp")),
            P("grp", ("blk", "tp")),
            P("grp", ("blk", "tp")),
            P("grp", ("blk", "tp")),
            P("grp", ("blk", "tp")),
            P("grp", ("blk", "tp")),
            P(),
            P(),
            P(("blk", "tp"), None),
            P("grp", ("blk", "tp")),
        ),
        out_specs=(
            P("grp", ("blk", "tp")),
            P("grp", ("blk", "tp")),
            P("grp", ("blk", "tp")),
            P("grp", ("blk", "tp")),
            P("grp", ("blk", "tp")),
            P("grp", ("blk", "tp")),
            P("grp", ("blk", "tp")),
            P(("blk", "tp"), "grp"),
        ),
        check_vma=False,
    )
```
